256 devices in a mesh: dp: 16 (over y, x), shard: 16 (over z, core).
Axes of the slice: x: 4, y: 4, z: 8, core: 2. Of those that a mesh axis runs over, the one named last changes fastest.
Arguments:
- gradients: bfloat16 [16, 12288, 2048], P('dp', 'shard'), may hold values from -4000 to 4000, as said below
- master_weights: float32 [12288, 2048], P(('shard', 'dp')), may hold values from -6 to 6
- first_moment: float32 [12288, 2048], P(('shard', 'dp')), may hold values from -4 to 4
- second_moment: float32 [12288, 2048], P(('shard', 'dp')), may hold values from 0.05 to 2
Outputs:
- parameters: bfloat16 [12288, 2048], P('shard')
- new_master: float32 [12288, 2048], P(('shard', 'dp'))
- new_first: float32 [12288, 2048], P(('shard', 'dp'))
- new_second: float32 [12288, 2048], P(('shard', 'dp'))
The draws below stay inside these ranges and needn't reach their ends.
Inputs may be any that keep to these rules, and one draw needn't show every extreme that they name: `gradients`: each replica's partial gradient.
All inputs are finite; a program needn't handle non-finite values.
Results may differ from the reference program's by a relative error of at most 0.006.
Values may be sent and summed in bfloat16 or wider, within the bound.
No kernel may reach another device: no remote copies, remote signals or barrier semaphores. Data moves between devices by JAX's collectives and lax.ppermute only.
A program may use at most 64 MiB of HBM per device.

```python
import math
import jax
import jax.numpy as jnp
from jax import lax

D = 2048
ROWS_DEV = 48
ROWS = 12288
N_DP = 16


def draw_gradients(key, part):
    keys = jax.random.split(jax.random.fold_in(key, 17), 7)
    shape = (N_DP, ROWS, D)
    groups = ROWS // ROWS_DEV
    group_of_row = jnp.arange(ROWS, dtype=jnp.int32) // ROWS_DEV
    common = jnp.clip(jax.random.normal(keys[5], (1, ROWS, D), jnp.float32), -5.0, 5.0)
    independent = jnp.clip(jax.random.normal(keys[0], shape, jnp.float32), -5.0, 5.0)
    agreement = jax.random.uniform(keys[4], (groups,), jnp.float32, -1.0, 2.0)
    base = independent + agreement[group_of_row][None, :, None] * common
    rise = jnp.arange(ROWS, dtype=jnp.float32) / max(ROWS - 1, 1)
    row_scale = jnp.exp(jax.random.uniform(keys[1], (ROWS,), jnp.float32) * math.log(10.0)) * jnp.exp(rise * math.log(3.0))
    col_scale = jnp.exp(jax.random.uniform(keys[2], (D,), jnp.float32) * math.log(10.0))
    group_keys = jax.random.split(keys[3], groups)
    order = jax.vmap(lambda one_key: jax.random.permutation(one_key, N_DP))(group_keys).astype(jnp.float32)
    rep_table = jnp.exp(order / max(N_DP - 1, 1) * math.log(3.0)) * jnp.exp(jax.random.uniform(keys[6], (groups, N_DP), jnp.float32) * 0.4)
    rep_scale = jnp.transpose(rep_table[group_of_row])
    values = base * row_scale[None, :, None] * col_scale[None, None, :] * rep_scale[:, :, None] * 0.1
    return values.astype(jnp.bfloat16)


def steps_of(own_key, shape, shards, least, top_value):
    level, own = 1.0, jax.random.fold_in(own_key, 6)
    for axis_at, blocks in shards:
        heights = jnp.exp(jax.random.uniform(jax.random.fold_in(own, axis_at), (blocks,), jnp.float32, least / len(shards), top_value / len(shards)))
        level = level * jnp.repeat(heights, shape[axis_at] // blocks).reshape([-1 if axis == axis_at else 1 for axis in range(len(shape))])
    return level


def centred(own_key, dims, scale, bound, shards=(), kind=jnp.bfloat16):
    gain = steps_of(own_key, dims, shards, -0.22, 0.18) if shards else 1.0
    drawn = jax.random.normal(own_key, dims, jnp.float32) * scale * gain
    return jnp.minimum(jnp.maximum(drawn, -bound), bound).astype(kind)


def setup_inputs(seed: int = 0) -> dict:
    key_list = jax.random.split(jax.random.key(seed), 5)
    gradients = draw_gradients(jax.random.fold_in(key_list[4], 71), 0)
    master_weights = centred(key_list[1], (ROWS, D), 1.0, 6.0, ((0, 256),), jnp.float32)
    first_moment = centred(key_list[2], (ROWS, D), 0.3, 4.0, ((0, 256),), jnp.float32)
    second_moment = jnp.clip(jnp.exp(math.log(2.0) - 3.6888794 * jax.random.uniform(key_list[3], (ROWS, D), jnp.float32) ** steps_of(key_list[3], (ROWS, D), ((0, 256),), -0.2, 0.2)), 0.05, 2.0)
    return dict(gradients=gradients, master_weights=master_weights, first_moment=first_moment, second_moment=second_moment)


first_bias = 1.0 - math.exp(100.0 * math.log(0.9))
second_bias = 1.0 - math.exp(100.0 * math.log(0.95))

def adam_update(summed, factor, master_weights, first_moment, second_moment):
    clipped = factor * summed
    new_first = 0.9 * first_moment + 0.1 * clipped
    new_second = 0.95 * second_moment + 0.05 * clipped * clipped
    first_hat = new_first / first_bias
    second_hat = new_second / second_bias
    new_master = master_weights - 0.01 * (first_hat / (jnp.sqrt(second_hat) + 1e-08) + 0.1 * master_weights)
    return (new_master, new_first, new_second)

def reference(gradients, master_weights, first_moment, second_moment):

    def accumulate(total, piece):
        return (total + piece.astype(jnp.float32), None)
    summed, unused = lax.scan(accumulate, jnp.zeros(gradients.shape[1:], jnp.float32), gradients)
    square_sum = jnp.sum(summed * summed)
    limit = 0.5 * math.sqrt(ROWS * D)
    factor = jnp.minimum(1.0, limit / jnp.sqrt(square_sum + 1e-06))
    new_master, new_first, new_second = adam_update(summed, factor, master_weights, first_moment, second_moment)
    parameters = new_master.astype(jnp.bfloat16)
    return (parameters, new_master, new_first, new_second)
```

```python
import math

import jax
import jax.numpy as jnp
from jax import lax
from jax.experimental import pallas as pl
from jax.experimental.pallas import tpu as pltpu
from jax.sharding import Mesh
from jax.sharding import PartitionSpec as P

DP = ("dp_0", "dp_1")
SHARD = ("shard_0", "shard_1")
SHARD_DP = ("shard_0", "shard_1", "dp_0", "dp_1")
PAIRED = ("dp_0", "dp_1", "shard_1")


first_bias = 1.0 - math.exp(100.0 * math.log(0.9))
second_bias = 1.0 - math.exp(100.0 * math.log(0.95))

ORDERS = (
    ((0, 1), (1, 1), (0, 3), (1, 3)),
    ((0, 3), (1, 3), (0, 1), (1, 1)),
)


def exchange(array, order, step):
    axis, flip = ORDERS[order][step]
    pairs = []
    for y in range(4):
        for x in range(4):
            for core in range(2):
                along_x = (axis == 0) == (core == 0)
                to_y, to_x = (y, x ^ flip) if along_x else (y ^ flip, x)
                pairs.append(((y * 4 + x) * 2 + core, (to_y * 4 + to_x) * 2 + core))
    return lax.ppermute(array, PAIRED, pairs)


def relative(order, number):
    offsets = [0, 0]
    for step in range(4):
        if (number >> (3 - step)) & 1:
            axis, flip = ORDERS[order][step]
            offsets[axis] ^= flip
    return offsets


def block_of(order, number):
    y, x, core = (lax.axis_index(name) for name in ("dp_0", "dp_1", "shard_1"))
    own, other = relative(order, number)
    off_x = jnp.where(core == 0, own, other)
    off_y = jnp.where(core == 0, other, own)
    return (y ^ off_y) * 4 + (x ^ off_x)


def picked(gradients, order, numbers, rows, half):
    def kernel(source, target, sems):
        copies = []
        for i, number in enumerate(numbers):
            at = pl.multiple_of(block_of(order, number) * rows, rows)
            copy = pltpu.make_async_copy(
                source.at[0, pl.ds(at, rows), pl.ds(order * half, half)],
                target.at[pl.ds(i * rows, rows)],
                sems.at[i],
            )
            copy.start()
            copies.append(copy)
        for copy in copies:
            copy.wait()

    count = len(numbers)
    return pl.pallas_call(
        kernel,
        out_shape=jax.ShapeDtypeStruct((count * rows, half), gradients.dtype),
        in_specs=[pl.BlockSpec(memory_space=pl.ANY)],
        out_specs=pl.BlockSpec(memory_space=pltpu.VMEM),
        scratch_shapes=[pltpu.SemaphoreType.DMA((count,))],
        cost_estimate=pl.CostEstimate(
            flops=2000000, bytes_accessed=4 * count * rows * half, transcendentals=0
        ),
        name=f"pick_{order}_{numbers[0]}",
    )(gradients)


def placed(pieces, numbers, rows, half, whole):
    def kernel(*refs):
        sources, target, sems = refs[:2], refs[-2], refs[-1]
        copies = []
        for order in range(2):
            for i, number in enumerate(numbers):
                at = pl.multiple_of(block_of(order, number) * rows, rows)
                copy = pltpu.make_async_copy(
                    sources[order].at[pl.ds(i * rows, rows)],
                    target.at[pl.ds(at, rows), pl.ds(order * half, half)],
                    sems.at[order * len(numbers) + i],
                )
                copy.start()
                copies.append(copy)
        for copy in copies:
            copy.wait()

    count = 2 * len(numbers)
    more = () if whole is None else (whole,)
    return pl.pallas_call(
        kernel,
        out_shape=jax.ShapeDtypeStruct((16 * rows, 2 * half), pieces[0].dtype),
        in_specs=[pl.BlockSpec(memory_space=pltpu.VMEM)] * 2
        + [pl.BlockSpec(memory_space=pl.ANY)] * len(more),
        out_specs=pl.BlockSpec(memory_space=pl.ANY),
        scratch_shapes=[pltpu.SemaphoreType.DMA((count,))],
        input_output_aliases={2: 0} if more else {},
        cost_estimate=pl.CostEstimate(
            flops=2000000, bytes_accessed=4 * count * rows * half, transcendentals=0
        ),
        name=f"place_{numbers[0]}",
    )(*pieces, *more)


def of_everyone(value, axes):
    size = lax.axis_size(axes)
    sent = jnp.broadcast_to(value[None, None, None], (size, 1, 1))
    return jnp.sum(lax.all_to_all(sent, axes, 0, 0, tiled=True))


def adam_update(summed, factor, master_weights, first_moment, second_moment):
    clipped = factor * summed
    new_first = 0.9 * first_moment + 0.1 * clipped
    new_second = 0.95 * second_moment + 0.05 * clipped * clipped
    first_hat = new_first / first_bias
    second_hat = new_second / second_bias
    new_master = master_weights - 0.01 * (
        first_hat / (jnp.sqrt(second_hat) + 1e-08) + 0.1 * master_weights
    )
    return (new_master, new_first, new_second)


def reduced(gradients, rows, half):
    f32 = jnp.float32
    away = [picked(gradients, o, range(8, 16), rows, half) for o in range(2)]
    totals = [None, None]
    for step in range(4):
        count = 8 >> step
        arrived = [exchange(away[o], o, step) for o in range(2)]
        if step == 0:
            totals = [
                picked(gradients, o, range(8), rows, half).astype(f32) for o in range(2)
            ]
        totals = [t + a.astype(f32) for t, a in zip(totals, arrived)]
        cut = count // 2 * rows
        if step < 3:
            away = [t[cut:].astype(jnp.bfloat16) for t in totals]
            totals = [t[:cut] for t in totals]
    return jnp.concatenate(totals, axis=1)


def gathered(owned, rows, half):
    held = [owned[:, :half], owned[:, half:]]
    for step in (3, 2, 1, 0):
        arrived = [exchange(held[o], o, step) for o in range(2)]
        if step:
            held = [jnp.concatenate([h, a]) for h, a in zip(held, arrived)]
    out = placed(held, range(8), rows, half, None)
    return placed(arrived, range(8, 16), rows, half, out)


def per_device(gradients, master_weights, first_moment, second_moment):
    rows, width = master_weights.shape
    half = width // 2
    entries = rows * lax.axis_size(DP) * lax.axis_size(SHARD) * width
    summed = reduced(gradients, rows, half)
    square_sum = of_everyone(of_everyone(jnp.sum(summed * summed), SHARD), DP)
    limit = 0.5 * math.sqrt(entries)
    factor = jnp.minimum(1.0, limit / jnp.sqrt(square_sum + 1e-06))
    new_master, new_first, new_second = adam_update(
        summed, factor, master_weights, first_moment, second_moment
    )
    parameters = gathered(new_master.astype(jnp.bfloat16), rows, half)
    return (parameters, new_master, new_first, new_second)


def solution(mesh):
    split = Mesh(mesh.devices.reshape(4, 4, 8, 2), ("dp_0", "dp_1", "shard_0", "shard_1"))
    return jax.shard_map(
        per_device,
        mesh=split,
        in_specs=(P(DP, SHARD, None), P(SHARD_DP, None), P(SHARD_DP, None), P(SHARD_DP, None)),
        out_specs=(P(SHARD, None), P(SHARD_DP, None), P(SHARD_DP, None), P(SHARD_DP, None)),
        check_vma=False,
    )
```

```python
import math

import jax
import jax.numpy as jnp
from jax import lax
from jax.experimental import pallas as pl
from jax.experimental.pallas import tpu as pltpu
from jax.sharding import Mesh
from jax.sharding import PartitionSpec as P

DP = ("dp_0", "dp_1")
SHARD = ("shard_0", "shard_1")
SHARD_DP = ("shard_0", "shard_1", "dp_0", "dp_1")
PAIRED = ("dp_0", "dp_1", "shard_1")
SIDE = 4


first_bias = 1.0 - math.exp(100.0 * math.log(0.9))
second_bias = 1.0 - math.exp(100.0 * math.log(0.95))


def moved(array, axis, by):
    pairs = []
    for y in range(SIDE):
        for x in range(SIDE):
            for core in range(2):
                to_y, to_x = (y, (x + by) % SIDE) if axis == core else ((y + by) % SIDE, x)
                pairs.append(((y * SIDE + x) * 2 + core, (to_y * SIDE + to_x) * 2 + core))
    return lax.ppermute(array, PAIRED, pairs)


def block_at(first, second):
    y, x, core = (lax.axis_index(name) for name in ("dp_0", "dp_1", "shard_1"))
    off_x = jnp.where(core == 0, first, second)
    off_y = jnp.where(core == 0, second, first)
    return lax.rem(y + off_y, SIDE) * SIDE + lax.rem(x + off_x, SIDE)


def picked(gradients, first, seconds, rows):
    width = gradients.shape[-1]

    def kernel(source, target, sems):
        copies = []
        for i, second in enumerate(seconds):
            at = pl.multiple_of(block_at(first, second) * rows, rows)
            copy = pltpu.make_async_copy(
                source.at[0, pl.ds(at, rows)], target.at[pl.ds(i * rows, rows)], sems.at[i]
            )
            copy.start()
            copies.append(copy)
        for copy in copies:
            copy.wait()

    count = len(seconds)
    return pl.pallas_call(
        kernel,
        out_shape=jax.ShapeDtypeStruct((count * rows, width), gradients.dtype),
        in_specs=[pl.BlockSpec(memory_space=pltpu.HBM)],
        out_specs=pl.BlockSpec(memory_space=pl.ANY),
        scratch_shapes=[pltpu.SemaphoreType.DMA((count,))],
        compiler_params=pltpu.CompilerParams(vmem_limit_bytes=1 << 20),
        cost_estimate=pl.CostEstimate(
            flops=2000000, bytes_accessed=4 * count * rows * width, transcendentals=0
        ),
    )(gradients)


def placed(pieces, places, rows, whole):
    width = pieces[0].shape[-1]
    count = sum(len(p) for p in places)

    def kernel(*refs):
        target, sems = refs[-2:]
        copies = []
        for source, own_places in zip(refs, places):
            for i, (first, second) in enumerate(own_places):
                at = pl.multiple_of(block_at(first, second) * rows, rows)
                copy = pltpu.make_async_copy(
                    source.at[pl.ds(i * rows, rows)],
                    target.at[pl.ds(at, rows)],
                    sems.at[len(copies)],
                )
                copy.start()
                copies.append(copy)
        for copy in copies:
            copy.wait()

    more = () if whole is None else (whole,)
    return pl.pallas_call(
        kernel,
        out_shape=jax.ShapeDtypeStruct((SIDE * SIDE * rows, width), pieces[0].dtype),
        in_specs=[pl.BlockSpec(memory_space=pl.ANY)] * (len(pieces) + len(more)),
        out_specs=pl.BlockSpec(memory_space=pl.ANY),
        scratch_shapes=[pltpu.SemaphoreType.DMA((count,))],
        input_output_aliases={len(pieces): 0} if more else {},
        compiler_params=pltpu.CompilerParams(vmem_limit_bytes=1 << 20),
        cost_estimate=pl.CostEstimate(
            flops=2000000, bytes_accessed=4 * count * rows * width, transcendentals=0
        ),
    )(*pieces, *more)


def of_everyone(partial, axes):
    size = lax.axis_size(axes)
    sent = jnp.broadcast_to(partial[None], (size, *partial.shape))
    return lax.all_to_all(sent, axes, 0, 0, tiled=True)


def adam_update(summed, factor, master_weights, first_moment, second_moment):
    clipped = factor * summed
    new_first = 0.9 * first_moment + 0.1 * clipped
    new_second = 0.95 * second_moment + 0.05 * clipped * clipped
    first_hat = new_first / first_bias
    second_hat = new_second / second_bias
    new_master = master_weights - 0.01 * (
        first_hat / (jnp.sqrt(second_hat) + 1e-08) + 0.1 * master_weights
    )
    return (new_master, new_first, new_second)


def reduced(gradients, rows):
    f32 = jnp.float32
    onward = range(1, SIDE)
    passing = {}
    for d in (2, 1, 3):
        passing[d] = moved(picked(gradients, d, onward, rows), 0, d).astype(f32)
    staying = {}
    for d in (2, 1, 3):
        staying[d] = moved(picked(gradients, d, (0,), rows), 0, d).astype(f32)
    total = picked(gradients, 0, onward, rows).astype(f32) + sum(passing.values())
    arrived = {}
    for e in (2, 1, 3):
        piece = total[(e - 1) * rows : e * rows].astype(jnp.bfloat16)
        arrived[e] = moved(piece, 1, e).astype(f32)
    own = picked(gradients, 0, (0,), rows).astype(f32) + sum(staying.values())
    return own + sum(arrived.values())


def gathered(owned, rows):
    nearby = {e: moved(owned, 1, e) for e in (2, 1, 3)}
    along = {d: moved(owned, 0, d) for d in (2, 1, 3)}
    held = jnp.concatenate([nearby[e] for e in (1, 2, 3)])
    rest = {d: moved(held, 0, d) for d in (2, 1, 3)}
    early = [owned] + [nearby[e] for e in (1, 2, 3)] + [along[d] for d in (1, 2, 3)]
    places = [[(0, 0)]] + [[(0, -e)] for e in (1, 2, 3)] + [[(-d, 0)] for d in (1, 2, 3)]
    places = [[(f % SIDE, s % SIDE) for f, s in p] for p in places]
    out = placed(early, places, rows, None)
    late = [rest[d] for d in (1, 2, 3)]
    places = [[(-d % SIDE, -e % SIDE) for e in (1, 2, 3)] for d in (1, 2, 3)]
    return placed(late, places, rows, out)


def step(gradients, master_weights, first_moment, second_moment):
    rows, width = master_weights.shape
    entries = rows * lax.axis_size(DP) * lax.axis_size(SHARD) * width
    summed = reduced(gradients, rows)
    partial = jnp.sum(jnp.sum(summed * summed, axis=0).reshape(16, width // 16), axis=0)
    partial = jnp.sum(of_everyone(partial[None], SHARD), axis=0)
    square_sum = jnp.sum(of_everyone(partial, DP), axis=(0, 2))[:, None]
    limit = 0.5 * math.sqrt(entries)
    factor = jnp.minimum(1.0, limit / jnp.sqrt(square_sum + 1e-06))
    new_master, new_first, new_second = adam_update(
        summed, factor, master_weights, first_moment, second_moment
    )
    parameters = gathered(new_master.astype(jnp.bfloat16), rows)
    return (parameters, new_master, new_first, new_second)


def solution(mesh):
    split = Mesh(mesh.devices.reshape(4, 4, 8, 2), ("dp_0", "dp_1", "shard_0", "shard_1"))
    return jax.shard_map(
        step,
        mesh=split,
        in_specs=(P(DP, SHARD, None), P(SHARD_DP, None), P(SHARD_DP, None), P(SHARD_DP, None)),
        out_specs=(P(SHARD, None), P(SHARD_DP, None), P(SHARD_DP, None), P(SHARD_DP, None)),
        check_vma=False,
    )
```

```python
import math

import jax
import jax.numpy as jnp
from jax import lax
from jax.experimental import pallas as pl
from jax.experimental.pallas import tpu as pltpu
from jax.sharding import Mesh
from jax.sharding import PartitionSpec as P

DP = ("dp_0", "dp_1")
SHARD = ("shard_0", "shard_1")
SHARD_DP = ("shard_0", "shard_1", "dp_0", "dp_1")
PAIRED = ("dp_0", "dp_1", "shard_1")
SIDE = 4


first_bias = 1.0 - math.exp(100.0 * math.log(0.9))
second_bias = 1.0 - math.exp(100.0 * math.log(0.95))


def moved(array, axis, by):
    pairs = []
    for y in range(SIDE):
        for x in range(SIDE):
            for core in range(2):
                to_y, to_x = (y, (x + by) % SIDE) if axis == core else ((y + by) % SIDE, x)
                pairs.append(((y * SIDE + x) * 2 + core, (to_y * SIDE + to_x) * 2 + core))
    return lax.ppermute(array, PAIRED, pairs)


def block_at(first, second):
    y, x, core = (lax.axis_index(name) for name in ("dp_0", "dp_1", "shard_1"))
    off_x = jnp.where(core == 0, first, second)
    off_y = jnp.where(core == 0, second, first)
    return lax.rem(y + off_y, SIDE) * SIDE + lax.rem(x + off_x, SIDE)


def picked(gradients, first, seconds, rows, limit=1 << 20):
    width = gradients.shape[-1]

    def kernel(source, target, sems):
        copies = []
        for i, second in enumerate(seconds):
            at = pl.multiple_of(block_at(first, second) * rows, rows)
            copy = pltpu.make_async_copy(
                source.at[0, pl.ds(at, rows)], target.at[pl.ds(i * rows, rows)], sems.at[i]
            )
            copy.start()
            copies.append(copy)
        for copy in copies:
            copy.wait()

    count = len(seconds)
    return pl.pallas_call(
        kernel,
        out_shape=jax.ShapeDtypeStruct((count * rows, width), gradients.dtype),
        in_specs=[pl.BlockSpec(memory_space=pltpu.HBM)],
        out_specs=pl.BlockSpec(memory_space=pl.ANY),
        scratch_shapes=[pltpu.SemaphoreType.DMA((count,))],
        compiler_params=pltpu.CompilerParams(vmem_limit_bytes=limit),
        cost_estimate=pl.CostEstimate(
            flops=2000000, bytes_accessed=4 * count * rows * width, transcendentals=0
        ),
    )(gradients)


def placed(pieces, places, rows, whole):
    width = pieces[0].shape[-1]
    count = sum(len(p) for p in places)

    def kernel(*refs):
        target, sems = refs[-2:]
        copies = []
        for source, own_places in zip(refs, places):
            for i, (first, second) in enumerate(own_places):
                at = pl.multiple_of(block_at(first, second) * rows, rows)
                copy = pltpu.make_async_copy(
                    source.at[pl.ds(i * rows, rows)],
                    target.at[pl.ds(at, rows)],
                    sems.at[len(copies)],
                )
                copy.start()
                copies.append(copy)
        for copy in copies:
            copy.wait()

    more = () if whole is None else (whole,)
    return pl.pallas_call(
        kernel,
        out_shape=jax.ShapeDtypeStruct((SIDE * SIDE * rows, width), pieces[0].dtype),
        in_specs=[pl.BlockSpec(memory_space=pl.ANY)] * (len(pieces) + len(more)),
        out_specs=pl.BlockSpec(memory_space=pl.ANY),
        scratch_shapes=[pltpu.SemaphoreType.DMA((count,))],
        input_output_aliases={len(pieces): 0} if more else {},
        compiler_params=pltpu.CompilerParams(vmem_limit_bytes=1 << 20),
        cost_estimate=pl.CostEstimate(
            flops=2000000, bytes_accessed=4 * count * rows * width, transcendentals=0
        ),
    )(*pieces, *more)


def of_everyone(partial, axes):
    size = lax.axis_size(axes)
    sent = jnp.broadcast_to(partial[None], (size, *partial.shape))
    return lax.all_to_all(sent, axes, 0, 0, tiled=True)


def adam_update(summed, factor, master_weights, first_moment, second_moment):
    clipped = factor * summed
    new_first = 0.9 * first_moment + 0.1 * clipped
    new_second = 0.95 * second_moment + 0.05 * clipped * clipped
    first_hat = new_first / first_bias
    second_hat = new_second / second_bias
    new_master = master_weights - 0.01 * (
        first_hat / (jnp.sqrt(second_hat) + 1e-08) + 0.1 * master_weights
    )
    return (new_master, new_first, new_second)


def factor_of(square_sums, entries):
    limit = 0.5 * math.sqrt(entries)
    square_sum = jnp.sum(square_sums, axis=(0, 2))[:, None]
    return jnp.minimum(1.0, limit / jnp.sqrt(square_sum + 1e-06))


def updated(square_sums, entries, summed, *state, parameters):
    def kernel(squares, summed, master, first, second, *outs):
        factor = factor_of(squares[...], entries)
        new = adam_update(summed[...], factor, master[...], first[...], second[...])
        for out, value in zip(outs, new):
            out[...] = value.astype(out.dtype)

    vmem = pl.BlockSpec(memory_space=pltpu.VMEM)
    dtypes = (jnp.bfloat16,) if parameters else (jnp.float32,) * 3
    return pl.pallas_call(
        kernel,
        out_shape=[jax.ShapeDtypeStruct(summed.shape, dtype) for dtype in dtypes],
        in_specs=[vmem] * 5,
        out_specs=[vmem] * len(dtypes),
        compiler_params=pltpu.CompilerParams(vmem_limit_bytes=8 << 20),
        cost_estimate=pl.CostEstimate(
            flops=2000000, bytes_accessed=18 * summed.size, transcendentals=2 * summed.size
        ),
        name="owned_parameters" if parameters else "new_state",
    )(square_sums, summed, *state)


def reduced(gradients, rows):
    f32 = jnp.float32
    onward = range(1, SIDE)
    passing = {}
    for d in (2, 1, 3):
        limit = 55000000 if d == 2 else 1 << 20
        block = picked(gradients, d, onward, rows, limit)
        passing[d] = moved(block, 0, d).astype(f32)
    staying = {}
    for d in (2, 1, 3):
        staying[d] = moved(picked(gradients, d, (0,), rows), 0, d).astype(f32)
    total = picked(gradients, 0, onward, rows).astype(f32) + sum(passing.values())
    arrived = {}
    for e in (2, 1, 3):
        piece = total[(e - 1) * rows : e * rows].astype(jnp.bfloat16)
        arrived[e] = moved(piece, 1, e).astype(f32)
    own = picked(gradients, 0, (0,), rows).astype(f32) + sum(staying.values())
    return own + sum(arrived.values())


def gathered(owned, rows):
    near = {e: moved(owned, 1, e) for e in (2, 1, 3)}
    halves = ((0, 1), (2, 3))
    blocks = {0: owned, **near}
    held = [jnp.concatenate([blocks[e] for e in half]) for half in halves]
    fore, back = [None] * 2, [None] * 2
    for at in range(2):
        fore[at] = moved(held[at], 0, 1)
        back[1 - at] = moved(held[1 - at], 0, 3)
    far = [moved(fore[0], 0, 1), moved(back[1], 0, 3)]

    def places(first, half):
        return [(first % SIDE, -e % SIDE) for e in halves[half]]

    out = None
    for pieces in (
        [(held[0], 0, 0), (held[1], 0, 1), (fore[0], -1, 0), (back[1], 1, 1)],
        [(fore[1], -1, 1), (back[0], 1, 0)],
        [(far[0], -2, 0), (far[1], 2, 1)],
    ):
        at = [places(first, half) for _, first, half in pieces]
        out = placed([piece for piece, _, _ in pieces], at, rows, out)
    return out


def step(gradients, master_weights, first_moment, second_moment):
    rows, width = master_weights.shape
    entries = rows * lax.axis_size(DP) * lax.axis_size(SHARD) * width
    summed = reduced(gradients, rows)
    partial = jnp.sum(jnp.sum(summed * summed, axis=0).reshape(16, width // 16), axis=0)
    partial = jnp.sum(of_everyone(partial[None], SHARD), axis=0)
    squares = of_everyone(partial, DP)
    state = (master_weights, first_moment, second_moment)
    inputs = (squares, entries, summed, *state)
    (owned,) = updated(*inputs, parameters=True)
    parameters = gathered(owned, rows)
    return (parameters, *updated(*inputs, parameters=False))


def solution(mesh):
    split = Mesh(mesh.devices.reshape(4, 4, 8, 2), ("dp_0", "dp_1", "shard_0", "shard_1"))
    return jax.shard_map(
        step,
        mesh=split,
        in_specs=(P(DP, SHARD, None), P(SHARD_DP, None), P(SHARD_DP, None), P(SHARD_DP, None)),
        out_specs=(P(SHARD, None), P(SHARD_DP, None), P(SHARD_DP, None), P(SHARD_DP, None)),
        check_vma=False,
    )
```

```python
import math

import jax
import jax.numpy as jnp
from jax import lax
from jax.experimental import pallas as pl
from jax.experimental.pallas import tpu as pltpu
from jax.sharding import Mesh
from jax.sharding import PartitionSpec as P

DP = ("dp_0", "dp_1")
SHARD = ("shard_0", "shard_1")
SHARD_DP = ("shard_0", "shard_1", "dp_0", "dp_1")
PAIRED = ("dp_0", "dp_1", "shard_1")
SIDE = 4
PIECE = 1024


first_bias = 1.0 - math.exp(100.0 * math.log(0.9))
second_bias = 1.0 - math.exp(100.0 * math.log(0.95))


def moved(array, axis, by):
    pairs = []
    for y in range(SIDE):
        for x in range(SIDE):
            for core in range(2):
                to_y, to_x = (y, x ^ by) if axis == core else (y ^ by, x)
                pairs.append(((y * SIDE + x) * 2 + core, (to_y * SIDE + to_x) * 2 + core))
    return lax.ppermute(array, PAIRED, pairs)


def block_at(first, second):
    y, x, core = (lax.axis_index(name) for name in ("dp_0", "dp_1", "shard_1"))
    off_x = jnp.where(core == 0, first, second)
    off_y = jnp.where(core == 0, second, first)
    return (y ^ off_y) * SIDE + (x ^ off_x)


def picked(gradients, first, seconds, rows, limit=1 << 20):
    width = gradients.shape[-1]

    def kernel(source, target, sems):
        copies = []
        for i, second in enumerate(seconds):
            at = pl.multiple_of(block_at(first, second) * rows, rows)
            for left in range(0, width, PIECE):
                copy = pltpu.make_async_copy(
                    source.at[0, pl.ds(at, rows), pl.ds(left, PIECE)],
                    target.at[pl.ds(i * rows, rows), pl.ds(left, PIECE)],
                    sems.at[len(copies)],
                )
                copy.start()
                copies.append(copy)
        for copy in copies:
            copy.wait()

    count = len(seconds)
    return pl.pallas_call(
        kernel,
        out_shape=jax.ShapeDtypeStruct((count * rows, width), gradients.dtype),
        in_specs=[pl.BlockSpec(memory_space=pltpu.HBM)],
        out_specs=pl.BlockSpec(memory_space=pl.ANY),
        scratch_shapes=[pltpu.SemaphoreType.DMA((count * (width // PIECE),))],
        compiler_params=pltpu.CompilerParams(vmem_limit_bytes=limit),
        cost_estimate=pl.CostEstimate(
            flops=2000000, bytes_accessed=4 * count * rows * width, transcendentals=0
        ),
    )(gradients)


def placed(pieces, places, rows, whole):
    width = pieces[0].shape[-1]
    count = sum(len(p) for p in places)

    def kernel(*refs):
        target, sems = refs[-2:]
        copies = []
        for source, own_places in zip(refs, places):
            for i, (first, second) in enumerate(own_places):
                at = pl.multiple_of(block_at(first, second) * rows, rows)
                copy = pltpu.make_async_copy(
                    source.at[pl.ds(i * rows, rows)],
                    target.at[pl.ds(at, rows)],
                    sems.at[len(copies)],
                )
                copy.start()
                copies.append(copy)
        for copy in copies:
            copy.wait()

    more = () if whole is None else (whole,)
    return pl.pallas_call(
        kernel,
        out_shape=jax.ShapeDtypeStruct((SIDE * SIDE * rows, width), pieces[0].dtype),
        in_specs=[pl.BlockSpec(memory_space=pl.ANY)] * (len(pieces) + len(more)),
        out_specs=pl.BlockSpec(memory_space=pl.ANY),
        scratch_shapes=[pltpu.SemaphoreType.DMA((count,))],
        input_output_aliases={len(pieces): 0} if more else {},
        compiler_params=pltpu.CompilerParams(vmem_limit_bytes=1 << 20),
        cost_estimate=pl.CostEstimate(
            flops=2000000, bytes_accessed=4 * count * rows * width, transcendentals=0
        ),
    )(*pieces, *more)


def of_everyone(partial, axes):
    size = lax.axis_size(axes)
    sent = jnp.broadcast_to(partial[None], (size, *partial.shape))
    return lax.all_to_all(sent, axes, 0, 0, tiled=True)


def adam_update(summed, factor, master_weights, first_moment, second_moment):
    clipped = factor * summed
    new_first = 0.9 * first_moment + 0.1 * clipped
    new_second = 0.95 * second_moment + 0.05 * clipped * clipped
    first_hat = new_first / first_bias
    second_hat = new_second / second_bias
    new_master = master_weights - 0.01 * (
        first_hat / (jnp.sqrt(second_hat) + 1e-08) + 0.1 * master_weights
    )
    return (new_master, new_first, new_second)


def factor_of(square_sums, entries):
    limit = 0.5 * math.sqrt(entries)
    square_sum = jnp.sum(square_sums, axis=(0, 2))[:, None]
    return jnp.minimum(1.0, limit / jnp.sqrt(square_sum + 1e-06))


def updated(square_sums, entries, summed, *state, parameters):
    def kernel(squares, summed, master, first, second, *outs):
        factor = factor_of(squares[...], entries)
        new = adam_update(summed[...], factor, master[...], first[...], second[...])
        for out, value in zip(outs, new):
            out[...] = value.astype(out.dtype)

    vmem = pl.BlockSpec(memory_space=pltpu.VMEM)
    dtypes = (jnp.bfloat16,) if parameters else (jnp.float32,) * 3
    return pl.pallas_call(
        kernel,
        out_shape=[jax.ShapeDtypeStruct(summed.shape, dtype) for dtype in dtypes],
        in_specs=[vmem] * 5,
        out_specs=[vmem] * len(dtypes),
        compiler_params=pltpu.CompilerParams(vmem_limit_bytes=8 << 20),
        cost_estimate=pl.CostEstimate(
            flops=2000000, bytes_accessed=18 * summed.size, transcendentals=2 * summed.size
        ),
        name="owned_parameters" if parameters else "new_state",
    )(square_sums, summed, *state)


def reduced(gradients, rows):
    f32 = jnp.float32
    onward = range(1, SIDE)
    passing = {}
    for d in (2, 1, 3):
        limit = 55000000 if d == 2 else 1 << 20
        block = picked(gradients, d, onward, rows, limit)
        passing[d] = moved(block, 0, d).astype(f32)
    staying = {}
    for d in (2, 1, 3):
        staying[d] = moved(picked(gradients, d, (0,), rows), 0, d).astype(f32)
    total = picked(gradients, 0, onward, rows).astype(f32) + sum(passing.values())
    arrived = {}
    for e in (2, 1, 3):
        piece = total[(e - 1) * rows : e * rows].astype(jnp.bfloat16)
        arrived[e] = moved(piece, 1, e).astype(f32)
    own = picked(gradients, 0, (0,), rows).astype(f32) + sum(staying.values())
    return own + sum(arrived.values())


def gathered(owned, rows):
    near = {e: moved(owned, 1, e) for e in (2, 1, 3)}
    halves = ((0, 1), (2, 3))
    blocks = {0: owned, **near}
    held = [jnp.concatenate([blocks[e] for e in half]) for half in halves]
    fore, back = [None] * 2, [None] * 2
    for at in range(2):
        fore[at] = moved(held[at], 0, 1)
        back[1 - at] = moved(held[1 - at], 0, 3)
    far = [moved(fore[0], 0, 3), moved(back[1], 0, 1)]

    def places(first, half):
        return [(first, e) for e in halves[half]]

    out = None
    for pieces in (
        [(held[0], 0, 0), (held[1], 0, 1), (fore[0], 1, 0), (back[1], 3, 1)],
        [(fore[1], 1, 1), (back[0], 3, 0)],
        [(far[0], 2, 0), (far[1], 2, 1)],
    ):
        at = [places(first, half) for _, first, half in pieces]
        out = placed([piece for piece, _, _ in pieces], at, rows, out)
    return out


def step(gradients, master_weights, first_moment, second_moment):
    rows, width = master_weights.shape
    entries = rows * lax.axis_size(DP) * lax.axis_size(SHARD) * width
    summed = reduced(gradients, rows)
    partial = jnp.sum(jnp.sum(summed * summed, axis=0).reshape(16, width // 16), axis=0)
    partial = jnp.sum(of_everyone(partial[None], SHARD), axis=0)
    squares = of_everyone(partial, DP)
    state = (master_weights, first_moment, second_moment)
    inputs = (squares, entries, summed, *state)
    (owned,) = updated(*inputs, parameters=True)
    parameters = gathered(owned, rows)
    return (parameters, *updated(*inputs, parameters=False))


def solution(mesh):
    split = Mesh(mesh.devices.reshape(4, 4, 8, 2), ("dp_0", "dp_1", "shard_0", "shard_1"))
    return jax.shard_map(
        step,
        mesh=split,
        in_specs=(P(DP, SHARD, None), P(SHARD_DP, None), P(SHARD_DP, None), P(SHARD_DP, None)),
        out_specs=(P(SHARD, None), P(SHARD_DP, None), P(SHARD_DP, None), P(SHARD_DP, None)),
        check_vma=False,
    )
```
